512 devices in a mesh: member: 64 (over z, x, y_lo), tensor: 8 (over y_hi, core).
Axes of the slice: x: 4, y: 8 (y_hi: 4, y_lo: 2; y = y_hi * 2 + y_lo), z: 8, core: 2. Of those that a mesh axis runs over, the one named last changes fastest.
Arguments:
- tokens: bfloat16 [3072, 5120], P('member', 'tensor'), may hold values from -6 to 6
- up_weight: bfloat16 [5120, 27648], P('tensor', 'member'), may hold values from -0.078125 to 0.078125
- left_factors: bfloat16 [768, 5120], P('member', 'tensor'), may hold values from -6 to 6
- right_factors: bfloat16 [768, 27648], P('tensor', 'member'), may hold values from -6 to 6
- fitness: float32 [192], replicated, may hold values from -0.6 to 0.6
Outputs:
- hidden: bfloat16 [3072, 27648], P('tensor', 'member')
- gradient: bfloat16 [5120, 27648], P('tensor', 'member')
The draws below stay inside these ranges and needn't reach their ends.
All inputs are finite; a program needn't handle non-finite values.
Results may differ from the reference program's by a relative error of at most 0.014.
Values may be sent and summed in bfloat16 or wider, within the bound.
No kernel may reach another device: no remote copies, remote signals or barrier semaphores. Data moves between devices by JAX's collectives and lax.ppermute only.
A program may use at most 64 MiB of HBM per device.

```python
import jax
import jax.numpy as jnp

D = 5120
FFN_HIDDEN = 27648
RANK = 4
MEMBER_TOKENS = 16
POPULATION_SIZE = 192
TOKEN_TOTAL = 3072
N_TENSOR = 8


def shard_levels(key, dims, cuts, least, high):
    loudness = 1.0
    for dim, shards_of in cuts:
        heights = jax.random.uniform(jax.random.fold_in(jax.random.fold_in(key, 6), dim), (shards_of,), jnp.float32, least / len(cuts), high / len(cuts))
        loudness = loudness * jnp.repeat(jnp.exp(heights), dims[dim] // shards_of).reshape((-1,) + (1,) * (len(dims) - 1 - dim))
    return loudness


def gaussian(own_key, dims, width, limit, pieces=(), held_as=jnp.bfloat16):
    drawn = width * jax.random.normal(own_key, dims, jnp.float32)
    if pieces:
        drawn = drawn * shard_levels(own_key, dims, pieces, -0.22, 0.18)
    return jnp.clip(drawn, -limit, limit).astype(held_as)


def setup_inputs(seed: int = 0) -> dict:
    key_of = jax.random.split(jax.random.key(seed), 6)
    return {
        "tokens": gaussian(key_of[0], (TOKEN_TOTAL, D), 1.0, 6.0, ((0, 64), (1, 8))),
        "up_weight": gaussian(key_of[1], (D, FFN_HIDDEN), D ** -0.5, 0.078125, ((0, 8), (1, 64))),
        "left_factors": gaussian(key_of[2], (POPULATION_SIZE * RANK, D), 1.0, 6.0, ((0, 64), (1, 8))),
        "right_factors": gaussian(key_of[3], (POPULATION_SIZE * RANK, FFN_HIDDEN), 1.0, 6.0, ((0, 8), (1, 64))),
        "fitness": gaussian(key_of[4], (POPULATION_SIZE,), 0.1, 0.6, (), jnp.float32),
    }


def reference(tokens, up_weight, left_factors, right_factors, fitness):
    noise_scale = 0.25 * D ** -0.5
    mixing = noise_scale * RANK ** -0.5
    block_span_width = D // N_TENSOR
    right_factor_wide = right_factors.astype(jnp.float32).reshape(POPULATION_SIZE, RANK, FFN_HIDDEN)
    hidden_sum = jnp.zeros((TOKEN_TOTAL, FFN_HIDDEN), jnp.float32)
    for tensor_block in range(N_TENSOR):
        lower = tensor_block * block_span_width
        token_columns = tokens[:, lower:lower + block_span_width]
        left_cols = left_factors[:, lower:lower + block_span_width]
        base_term = jnp.dot(token_columns, up_weight[lower:lower + block_span_width, :], preferred_element_type=jnp.float32)
        up_projection = jnp.einsum("uzg,uig->uzi", token_columns.astype(jnp.float32).reshape(POPULATION_SIZE, MEMBER_TOKENS, block_span_width),
                                left_cols.astype(jnp.float32).reshape(POPULATION_SIZE, RANK, block_span_width)).astype(jnp.bfloat16)
        lowrank_correction = jnp.einsum("djt,dty->djy", up_projection.astype(jnp.float32), right_factor_wide).reshape(TOKEN_TOTAL, FFN_HIDDEN)
        partial_value = (base_term + mixing * lowrank_correction).astype(jnp.bfloat16)
        hidden_sum = hidden_sum + partial_value.astype(jnp.float32)
    hidden = hidden_sum.astype(jnp.bfloat16)
    fit_rows = jnp.repeat(fitness, RANK)
    weighted = (fit_rows[:, None] * left_factors.astype(jnp.float32)).astype(jnp.bfloat16)
    gradient = jnp.dot(weighted.T, right_factors, preferred_element_type=jnp.float32)
    gradient = gradient * (1.0 / (POPULATION_SIZE * noise_scale * RANK ** 0.5))
    return hidden, gradient.astype(jnp.bfloat16)
```

```python
import itertools

import jax
import jax.numpy as jnp
from jax import lax
from jax.sharding import Mesh
from jax.sharding import PartitionSpec as P

D = 5120
RANK = 4
MEMBER_TOKENS = 16
POPULATION = 192
MEMBER = ("z", "x", "lo")
TENSOR = ("hi", "core")
SIGMA = 0.25 * D**-0.5
MIXING = SIGMA * RANK**-0.5
GRADIENT_SCALE = 1.0 / (POPULATION * SIGMA * RANK**0.5)


def shifted(array, axis, step):
    size = lax.axis_size(axis)
    return lax.ppermute(array, axis, [(k, (k + step) % size) for k in range(size)])


def gathered(array, axes):
    copies = jnp.broadcast_to(array, (lax.axis_size(axes), *array.shape))
    return lax.all_to_all(copies, axes, split_axis=0, concat_axis=0, tiled=True)


def wrapped(stack, start, sign=1):
    count = stack.shape[0]
    order = (start + sign * jnp.arange(count)) % count
    return jnp.take(stack, order, axis=0, mode="clip")


def dot_t(a, b):
    return lax.dot_general(a, b, (((1,), (1,)), ((), ())), preferred_element_type=jnp.float32)


def body(tokens, up_weight, left_factors, right_factors, fitness):
    f32, bf16 = jnp.float32, jnp.bfloat16
    hi, core, x = lax.axis_index("hi"), lax.axis_index("core"), lax.axis_index("x")
    rows, features = tokens.shape
    factors = left_factors.shape[0]
    columns = up_weight.shape[1]
    n_x, n_hi, n_z, n_lo = (lax.axis_size(a) for a in ("x", "hi", "z", "lo"))
    wide = -(-(n_x * columns + RANK) // 128) * 128

    weight = up_weight.T
    weight_after = shifted(weight, "x", -1)
    weight_before = shifted(weight, "x", 1)
    mine = jnp.concatenate([tokens, left_factors, jnp.zeros((4, features), bf16)], 0)
    near = gathered(mine, ("z", "lo"))
    half = columns // 2
    weight_far = jnp.concatenate(
        [
            shifted(weight_before[:half], "x", 1),
            shifted(weight_after[half:], "x", -1),
        ],
        0,
    )
    right_all = gathered(right_factors, TENSOR)
    near, right_all = lax.optimization_barrier((near, right_all))
    near_left = near[:, rows : rows + factors]
    weights = jnp.concatenate(
        [weight, weight_after, weight_far, weight_before, jnp.zeros((wide - n_x * columns, features), bf16)], 0
    )

    block = n_lo * rows
    token_blocks = near[:, :rows].reshape(n_hi, 2, block, features)
    left_blocks = near_left.reshape(n_hi, 2, n_lo * factors, features)
    row = lax.broadcasted_iota(jnp.int32, (n_hi * block, n_hi * n_lo * factors), 0)
    col = lax.broadcasted_iota(jnp.int32, (n_hi * block, n_hi * n_lo * factors), 1)
    same = row // MEMBER_TOKENS == col // RANK
    k = lax.broadcasted_iota(jnp.int32, (wide, n_hi * n_lo * factors), 1)
    c = lax.broadcasted_iota(jnp.int32, (wide, n_hi * n_lo * factors), 0)
    place = (c == n_x * columns + k % RANK).astype(bf16)

    def partial(side):
        some = wrapped(lax.dynamic_index_in_dim(token_blocks, side, 1, False), hi)
        lefts = wrapped(lax.dynamic_index_in_dim(left_blocks, side, 1, False), hi)
        some = some.reshape(n_hi * block, features)
        lefts = lefts.reshape(-1, features)
        projection = jnp.where(same, dot_t(some, lefts), 0.0).astype(bf16)
        return (dot_t(some, weights) + dot_t(projection, place)).reshape(n_hi, block, wide)

    sent = partial(1 - core).astype(bf16)
    other = shifted(sent, "core", 1)
    both = (partial(core) + other.astype(f32)).astype(bf16)
    cut = block // 2
    via_after = shifted(both[2, :cut], "hi", 1)
    via_before = shifted(both[2, cut:], "hi", -1)
    to_after = jnp.concatenate(
        [(both[1, :cut].astype(f32) + via_after.astype(f32)).astype(bf16), both[1, cut:]], 0
    )
    to_before = jnp.concatenate(
        [both[3, :cut], (both[3, cut:].astype(f32) + via_before.astype(f32)).astype(bf16)], 0
    )
    from_before = shifted(to_after, "hi", 1)
    from_after = shifted(to_before, "hi", -1)
    total = both[0].astype(f32) + from_before.astype(f32) + from_after.astype(f32)
    total = total.astype(bf16)

    pieces = []
    for j in range(n_x):
        piece = jnp.concatenate(
            [total[:, j * columns : (j + 1) * columns], total[:, n_x * columns : n_x * columns + RANK]], 1
        )
        pieces.append(shifted(piece, "x", j) if j else piece)
    whole = wrapped(jnp.stack(pieces), x, -1).reshape(n_x * block, columns + RANK)
    own = right_factors.shape[0]
    row = lax.broadcasted_iota(jnp.int32, (n_x * block, own), 0)
    col = lax.broadcasted_iota(jnp.int32, (n_x * block, own), 1)
    tiled = jnp.tile(whole[:, columns:], (1, own // RANK))
    spread = jnp.where(row // MEMBER_TOKENS == col // RANK, tiled, 0)
    correction = jnp.dot(spread, right_factors, preferred_element_type=f32)
    hidden = (whole[:, :columns].astype(f32) + MIXING * correction).astype(bf16)

    left_all = gathered(near_left, "x")
    left_all = left_all.reshape(n_x, n_z, n_lo * factors, features).transpose(1, 0, 2, 3)
    left_all = left_all.reshape(-1, features)
    fit = jnp.repeat(fitness, RANK)
    weighted = (fit[:, None] * left_all.astype(f32)).astype(bf16)
    right_all = right_all.reshape(-1, columns)
    gradient = jnp.einsum("kd,kf->df", weighted, right_all, preferred_element_type=f32)
    return hidden, (gradient * GRADIENT_SCALE).astype(bf16)


def solution(mesh):
    finer = Mesh(mesh.devices.reshape(8, 4, 2, 4, 2), MEMBER + TENSOR)
    return jax.shard_map(
        body,
        mesh=finer,
        in_specs=(P(MEMBER, TENSOR), P(TENSOR, MEMBER), P(MEMBER, TENSOR), P(TENSOR, MEMBER), P()),
        out_specs=(P(TENSOR, MEMBER), P(TENSOR, MEMBER)),
        check_vma=False,
    )
```

```python
import functools

import jax
import jax.numpy as jnp
from jax import lax
from jax.experimental import pallas as pl
from jax.experimental.pallas import tpu as pltpu
from jax.sharding import Mesh
from jax.sharding import PartitionSpec as P

D = 5120
RANK = 4
MEMBER_TOKENS = 16
POPULATION = 192
MEMBER = ("z", "x", "lo")
TENSOR = ("hi", "core")
SIGMA = 0.25 * D**-0.5
MIXING = SIGMA * RANK**-0.5
GRADIENT_SCALE = 1.0 / (POPULATION * SIGMA * RANK**0.5)


def shifted(array, axis, step):
    size = lax.axis_size(axis)
    return lax.ppermute(array, axis, [(k, (k + step) % size) for k in range(size)])


def gathered(array, axes):
    copies = jnp.broadcast_to(array, (lax.axis_size(axes), *array.shape))
    return lax.all_to_all(copies, axes, split_axis=0, concat_axis=0, tiled=True)


def wrapped(stack, start, sign=1):
    count = stack.shape[0]
    order = (start + sign * jnp.arange(count)) % count
    return jnp.take(stack, order, axis=0, mode="clip")


def dot_t(a, b):
    return lax.dot_general(a, b, (((1,), (1,)), ((), ())), preferred_element_type=jnp.float32)


CHUNK = 256


def partial_kernel(rows, factors, where_ref, *refs):
    *near_refs, weight_ref, out_ref, token_ref = refs
    step = pl.program_id(0)
    slot = near_refs[0].shape[1] // 2
    block = 2 * rows

    @pl.when(step == 0)
    def _():
        for j, near in enumerate(near_refs):
            token_ref[j * block : j * block + rows] = near[0, :rows]
            token_ref[j * block + rows : (j + 1) * block] = near[0, slot : slot + rows]

    product = dot_t(token_ref[...], weight_ref[...])

    @pl.when(step < pl.num_programs(0) - 1)
    def _():
        out_ref[...] = product.reshape(out_ref.shape).astype(out_ref.dtype)

    @pl.when(step == pl.num_programs(0) - 1)
    def _():
        row = lax.broadcasted_iota(jnp.int32, (block, 2 * slot), 0)
        col = lax.broadcasted_iota(jnp.int32, (block, 2 * slot), 1)
        place = col % slot - rows
        same = (row // rows == col // slot) & (place >= 0) & (place < factors)
        same &= row % rows // MEMBER_TOKENS == place // RANK
        k = lax.broadcasted_iota(jnp.int32, (2 * slot, 128), 0)
        c = lax.broadcasted_iota(jnp.int32, (2 * slot, 128), 1)
        pick = jnp.where(c == 64 + k % RANK, 1.0, 0.0).astype(jnp.bfloat16)
        for j, near in enumerate(near_refs):
            projection = dot_t(token_ref[j * block : (j + 1) * block], near[0])
            projection = jnp.where(same, projection, 0.0).astype(jnp.bfloat16)
            tail = jnp.dot(projection, pick, preferred_element_type=jnp.float32)
            part = product[j * block : (j + 1) * block]
            out_ref[j, :, :128] = part[:, :128].astype(out_ref.dtype)
            out_ref[j, :, 128:] = (part[:, 128:] + tail).astype(out_ref.dtype)


def partials(near, weights, where, rows, factors):
    n_hi = 4
    wide, features = weights.shape
    blocks = near.reshape(2 * n_hi, -1, features)

    def near_spec(j):
        return pl.BlockSpec((1, blocks.shape[1], features), lambda n, at: (2 * ((at[0] + j) % n_hi) + at[1], 0, 0))

    return pl.pallas_call(
        functools.partial(partial_kernel, rows, factors),
        grid_spec=pltpu.PrefetchScalarGridSpec(
            num_scalar_prefetch=1,
            grid=(wide // CHUNK,),
            in_specs=[near_spec(j) for j in range(n_hi)] + [pl.BlockSpec((CHUNK, features), lambda n, at: (n, 0))],
            out_specs=pl.BlockSpec((n_hi, 2 * rows, CHUNK), lambda n, at: (0, 0, n)),
            scratch_shapes=[pltpu.VMEM((n_hi * 2 * rows, features), jnp.bfloat16)],
        ),
        out_shape=jax.ShapeDtypeStruct((n_hi, 2 * rows, wide), jnp.bfloat16),
        cost_estimate=pl.CostEstimate(
            flops=2 * n_hi * 2 * rows * wide * features, transcendentals=0, bytes_accessed=2 * (wide * features + 2 * n_hi * rows * wide)
        ),
        compiler_params=pltpu.CompilerParams(dimension_semantics=("arbitrary",)),
    )(where, *[blocks] * n_hi, weights)


def body(tokens, up_weight, left_factors, right_factors, fitness):
    f32, bf16 = jnp.float32, jnp.bfloat16
    hi, core, x = lax.axis_index("hi"), lax.axis_index("core"), lax.axis_index("x")
    rows, features = tokens.shape
    factors = left_factors.shape[0]
    columns = up_weight.shape[1]
    own = right_factors.shape[0]
    n_x, n_hi, n_z, n_lo = (lax.axis_size(a) for a in ("x", "hi", "z", "lo"))
    wide = -(-(n_x * columns + RANK) // 128) * 128

    weight = up_weight.T
    weight_after = shifted(weight, "x", -1)
    weight_before = shifted(weight, "x", 1)
    mine = jnp.concatenate([tokens, left_factors, jnp.zeros((4, features), bf16)], 0)
    near = gathered(mine, ("z", "lo"))
    half = columns // 2
    weight_far = jnp.concatenate(
        [
            shifted(weight_before[:half], "x", 1),
            shifted(weight_after[half:], "x", -1),
        ],
        0,
    )
    right_after = shifted(right_factors, "hi", -1)
    right_before = shifted(right_factors, "hi", 1)
    low = own // 2
    right_far = jnp.concatenate([shifted(right_before[:low], "hi", 1), shifted(right_after[low:], "hi", -1)], 0)
    right_same = jnp.stack([right_factors, right_after, right_far, right_before])
    near, right_same = lax.optimization_barrier((near, right_same))
    near_left = near[:, rows : rows + factors]
    weights = jnp.concatenate(
        [weight, weight_after, weight_far, weight_before, jnp.zeros((wide - n_x * columns, features), bf16)], 0
    )

    block = n_lo * rows
    sent = partials(near, weights, jnp.stack([hi, 1 - core]), rows, factors)
    other = shifted(sent, "core", 1)
    kept = partials(near, weights, jnp.stack([hi, core]), rows, factors)
    both = (kept.astype(f32) + other.astype(f32)).astype(bf16)
    cut = block // 2
    via_after = shifted(both[2, :cut], "hi", 1)
    via_before = shifted(both[2, cut:], "hi", -1)
    to_after = jnp.concatenate(
        [(both[1, :cut].astype(f32) + via_after.astype(f32)).astype(bf16), both[1, cut:]], 0
    )
    to_before = jnp.concatenate(
        [both[3, :cut], (both[3, cut:].astype(f32) + via_before.astype(f32)).astype(bf16)], 0
    )
    from_before = shifted(to_after, "hi", 1)
    from_after = shifted(to_before, "hi", -1)
    total = both[0].astype(f32) + from_before.astype(f32) + from_after.astype(f32)
    total = total.astype(bf16)

    tail = total[:, n_x * columns : n_x * columns + RANK]
    pieces = [jnp.concatenate([total[:, j * columns : (j + 1) * columns], tail], 1) for j in range(n_x)]
    pieces = wrapped(jnp.stack(pieces), n_x - x)
    whole = lax.all_to_all(pieces, "x", split_axis=0, concat_axis=0, tiled=True)
    whole = whole.reshape(n_x * block, columns + RANK)
    row = lax.broadcasted_iota(jnp.int32, (n_x * block, own), 0)
    col = lax.broadcasted_iota(jnp.int32, (n_x * block, own), 1)
    tiled = jnp.tile(whole[:, columns:], (1, own // RANK))
    spread = jnp.where(row // MEMBER_TOKENS == col // RANK, tiled, 0)
    correction = jnp.dot(spread, right_factors, preferred_element_type=f32)
    hidden = (whole[:, :columns].astype(f32) + MIXING * correction).astype(bf16)

    left_all = gathered(near_left, "x")
    left_all = left_all.reshape(n_x, n_z, n_lo * factors, features).transpose(1, 0, 2, 3)
    left_all = left_all.reshape(-1, features)
    fit = jnp.repeat(fitness, RANK)
    weighted = (fit[:, None] * left_all.astype(f32)).astype(bf16)
    right_other = shifted(right_same, "core", 1)
    here = core == 0
    right_all = jnp.stack([jnp.where(here, right_same, right_other), jnp.where(here, right_other, right_same)], 1)
    right_all = wrapped(right_all, n_hi - hi).reshape(-1, columns)
    gradient = jnp.einsum("kd,kf->df", weighted, right_all, preferred_element_type=f32)
    return hidden, (gradient * GRADIENT_SCALE).astype(bf16)


def solution(mesh):
    finer = Mesh(mesh.devices.reshape(8, 4, 2, 4, 2), MEMBER + TENSOR)
    return jax.shard_map(
        body,
        mesh=finer,
        in_specs=(P(MEMBER, TENSOR), P(TENSOR, MEMBER), P(MEMBER, TENSOR), P(TENSOR, MEMBER), P()),
        out_specs=(P(TENSOR, MEMBER), P(TENSOR, MEMBER)),
        check_vma=False,
    )
```

```python
import functools

import jax
import jax.numpy as jnp
from jax import lax
from jax.experimental import pallas as pl
from jax.experimental.pallas import tpu as pltpu
from jax.sharding import Mesh
from jax.sharding import PartitionSpec as P

D = 5120
RANK = 4
MEMBER_TOKENS = 16
POPULATION = 192
MEMBER = ("z", "x", "lo")
TENSOR = ("hi", "core")
SIGMA = 0.25 * D**-0.5
MIXING = SIGMA * RANK**-0.5
GRADIENT_SCALE = 1.0 / (POPULATION * SIGMA * RANK**0.5)


def shifted(array, axis, step):
    size = lax.axis_size(axis)
    return lax.ppermute(array, axis, [(k, (k + step) % size) for k in range(size)])


def gathered(array, axes):
    copies = jnp.broadcast_to(array, (lax.axis_size(axes), *array.shape))
    return lax.all_to_all(copies, axes, split_axis=0, concat_axis=0, tiled=True)


def wrapped(stack, start, sign=1):
    count = stack.shape[0]
    order = (start + sign * jnp.arange(count)) % count
    return jnp.take(stack, order, axis=0, mode="clip")


def dot_t(a, b):
    return lax.dot_general(a, b, (((1,), (1,)), ((), ())), preferred_element_type=jnp.float32)


CHUNK = 256


def partial_kernel(rows, factors, where_ref, near_ref, weight_ref, sent_ref, kept_ref, token_ref, left_ref):
    slot = near_ref.shape[1] // 2
    block = 2 * rows
    n_hi = sent_ref.shape[0]
    wide, features = weight_ref.shape
    for side in range(2):
        for j in range(n_hi):
            z = 2 * ((where_ref[0] + j) % n_hi) + (where_ref[1] if side else 1 - where_ref[1])
            at = (side * n_hi + j) * block
            token_ref[at : at + rows] = near_ref[z, :rows]
            token_ref[at + rows : at + block] = near_ref[z, slot : slot + rows]
            left_ref[side * n_hi + j] = near_ref[z]
    row = lax.broadcasted_iota(jnp.int32, (block, 2 * slot), 0)
    col = lax.broadcasted_iota(jnp.int32, (block, 2 * slot), 1)
    place = col % slot - rows
    same = (row // rows == col // slot) & (place >= 0) & (place < factors)
    same &= row % rows // MEMBER_TOKENS == place // RANK
    k = lax.broadcasted_iota(jnp.int32, (2 * slot, CHUNK), 0)
    c = lax.broadcasted_iota(jnp.int32, (2 * slot, CHUNK), 1)
    pick = jnp.where(c == CHUNK - 64 + k % RANK, 1.0, 0.0).astype(jnp.bfloat16)
    for n in range(0, wide, CHUNK):
        for side, out_ref in enumerate((sent_ref, kept_ref)):
            some = token_ref[side * n_hi * block : (side + 1) * n_hi * block]
            product = dot_t(some, weight_ref[n : n + CHUNK]).reshape(n_hi, block, CHUNK)
            if n + CHUNK < wide:
                out_ref[:, :, n : n + CHUNK] = product.astype(out_ref.dtype)
                continue
            for j in range(n_hi):
                projection = dot_t(some[j * block : (j + 1) * block], left_ref[side * n_hi + j])
                projection = jnp.where(same, projection, 0.0).astype(jnp.bfloat16)
                tail = jnp.dot(projection, pick, preferred_element_type=jnp.float32)
                out_ref[j, :, n : n + CHUNK] = (product[j] + tail).astype(out_ref.dtype)


def partials(near, weights, where, rows, factors):
    n_hi = 4
    wide, features = weights.shape
    blocks = near.reshape(2 * n_hi, -1, features)
    block = 2 * rows
    vmem = pl.BlockSpec(memory_space=pltpu.VMEM)
    half = jax.ShapeDtypeStruct((n_hi, block, wide), jnp.bfloat16)
    return pl.pallas_call(
        functools.partial(partial_kernel, rows, factors),
        in_specs=[pl.BlockSpec(memory_space=pltpu.SMEM), vmem, vmem],
        out_specs=[vmem, vmem],
        out_shape=[half, half],
        scratch_shapes=[
            pltpu.VMEM((2 * n_hi * block, features), jnp.bfloat16),
            pltpu.VMEM((2 * n_hi, *blocks.shape[1:]), jnp.bfloat16),
        ],
        cost_estimate=pl.CostEstimate(
            flops=4 * n_hi * block * wide * features,
            transcendentals=0,
            bytes_accessed=2 * (wide * features + blocks.size + 2 * n_hi * block * wide),
        ),
    )(where, blocks, weights)


def body(tokens, up_weight, left_factors, right_factors, fitness):
    f32, bf16 = jnp.float32, jnp.bfloat16
    hi, core, x = lax.axis_index("hi"), lax.axis_index("core"), lax.axis_index("x")
    rows, features = tokens.shape
    factors = left_factors.shape[0]
    columns = up_weight.shape[1]
    own = right_factors.shape[0]
    n_x, n_hi, n_z, n_lo = (lax.axis_size(a) for a in ("x", "hi", "z", "lo"))
    wide = -(-(n_x * columns + RANK) // 128) * 128

    weight = up_weight.T
    weight_after = shifted(weight, "x", -1)
    weight_before = shifted(weight, "x", 1)
    mine = jnp.concatenate([tokens, left_factors, jnp.zeros((4, features), bf16)], 0)
    near = gathered(mine, ("z", "lo"))
    weight_far = shifted(weight, "x", 2)
    right_after = shifted(right_factors, "hi", -1)
    right_before = shifted(right_factors, "hi", 1)
    right_far = shifted(right_factors, "hi", 2)
    right_same = jnp.stack([right_factors, right_after, right_far, right_before])
    near, right_same = lax.optimization_barrier((near, right_same))
    near_left = near[:, rows : rows + factors]
    weights = jnp.concatenate(
        [weight, weight_after, weight_far, weight_before, jnp.zeros((wide - n_x * columns, features), bf16)], 0
    )

    block = n_lo * rows
    sent, kept = partials(near, weights, jnp.stack([hi, core]), rows, factors)
    other = shifted(sent, "core", 1)

    def both(j, start, stop):
        return kept[j, start:stop].astype(f32) + other[j, start:stop].astype(f32)

    cut = block // 2
    far_after = shifted(both(2, 0, cut).astype(bf16), "hi", 1)
    far_before = shifted(both(2, cut, block).astype(bf16), "hi", -1)
    high_before = shifted(both(1, cut, block).astype(bf16), "hi", 1)
    low_after = shifted(both(3, 0, cut).astype(bf16), "hi", -1)
    low_before = shifted((both(1, 0, cut) + far_after.astype(f32)).astype(bf16), "hi", 1)
    high_after = shifted((both(3, cut, block) + far_before.astype(f32)).astype(bf16), "hi", -1)
    low = both(0, 0, cut) + low_before.astype(f32) + low_after.astype(f32)
    high = both(0, cut, block) + high_before.astype(f32) + high_after.astype(f32)
    total = jnp.concatenate([low, high], 0).astype(bf16)

    tail = total[:, n_x * columns : n_x * columns + RANK]
    pieces = [jnp.concatenate([total[:, j * columns : (j + 1) * columns], tail], 1) for j in range(n_x)]
    pieces = wrapped(jnp.stack(pieces), n_x - x)
    whole = lax.all_to_all(pieces, "x", split_axis=0, concat_axis=0, tiled=True)
    whole = whole.reshape(n_x * block, columns + RANK)
    row = lax.broadcasted_iota(jnp.int32, (n_x * block, own), 0)
    col = lax.broadcasted_iota(jnp.int32, (n_x * block, own), 1)
    tiled = jnp.tile(whole[:, columns:], (1, own // RANK))
    spread = jnp.where(row // MEMBER_TOKENS == col // RANK, tiled, 0)
    correction = jnp.dot(spread, right_factors, preferred_element_type=f32)
    hidden = (whole[:, :columns].astype(f32) + MIXING * correction).astype(bf16)

    left_all = gathered(near_left, "x")
    left_all = left_all.reshape(n_x, n_z, n_lo * factors, features).transpose(1, 0, 2, 3)
    left_all = left_all.reshape(-1, features)
    fit = jnp.repeat(fitness, RANK)
    weighted = (fit[:, None] * left_all.astype(f32)).astype(bf16)
    right_other = shifted(right_same, "core", 1)
    here = core == 0
    right_all = jnp.stack([jnp.where(here, right_same, right_other), jnp.where(here, right_other, right_same)], 1)
    right_all = wrapped(right_all, n_hi - hi).reshape(-1, columns)
    gradient = jnp.einsum("kd,kf->df", weighted, right_all, preferred_element_type=f32)
    return hidden, (gradient * GRADIENT_SCALE).astype(bf16)


def solution(mesh):
    finer = Mesh(mesh.devices.reshape(8, 4, 2, 4, 2), MEMBER + TENSOR)
    return jax.shard_map(
        body,
        mesh=finer,
        in_specs=(P(MEMBER, TENSOR), P(TENSOR, MEMBER), P(MEMBER, TENSOR), P(TENSOR, MEMBER), P()),
        out_specs=(P(TENSOR, MEMBER), P(TENSOR, MEMBER)),
        check_vma=False,
    )
```

```python
import functools

import jax
import jax.numpy as jnp
import numpy as np
from jax import lax
from jax.experimental import pallas as pl
from jax.experimental.pallas import tpu as pltpu
from jax.sharding import Mesh
from jax.sharding import PartitionSpec as P


D = 5120
RANK = 4
MEMBER_TOKENS = 16
POPULATION = 192
MEMBER = ("z", "x", "lo")
TENSOR = ("hi", "core")
SIGMA = 0.25 * D**-0.5
MIXING = SIGMA * RANK**-0.5
GRADIENT_SCALE = 1.0 / (POPULATION * SIGMA * RANK**0.5)


def shifted(array, axis, step):
    size = lax.axis_size(axis)
    return lax.ppermute(array, axis, [(k, (k + step) % size) for k in range(size)])


def gathered(array, axes):
    copies = jnp.broadcast_to(array, (lax.axis_size(axes), *array.shape))
    return lax.all_to_all(copies, axes, split_axis=0, concat_axis=0, tiled=True)


def dot_t(a, b):
    return lax.dot_general(a, b, (((1,), (1,)), ((), ())), preferred_element_type=jnp.float32)


CHUNK = 256
LANES = 128


def partial_kernel(rows, factors, where_ref, near_hbm, *refs):
    *weight_hbm, sent_hbm, kept_hbm, left_hbm, near_ref, weight_ref, token_ref, left_ref, tail_ref, out_ref, in_sems, out_sems = refs
    slot = near_ref.shape[1] // 2
    block = 2 * rows
    n_hi = out_ref.shape[1]
    wide, features = weight_ref.shape
    columns = weight_hbm[0].shape[0]
    loads = [pltpu.make_async_copy(near_hbm, near_ref, in_sems.at[0])]
    for j, some in enumerate(weight_hbm):
        place = lax.rem(where_ref[2] + j, len(weight_hbm))
        part = weight_ref.at[pl.ds(pl.multiple_of(place * columns, 16), columns)]
        loads.append(pltpu.make_async_copy(some, part, in_sems.at[1 + place]))
    for load in loads:
        load.start()
    weight_ref[len(weight_hbm) * columns :] = jnp.zeros((wide - len(weight_hbm) * columns, features), jnp.bfloat16)
    row = lax.broadcasted_iota(jnp.int32, (block, 2 * slot), 0)
    col = lax.broadcasted_iota(jnp.int32, (block, 2 * slot), 1)
    place = col % slot - rows
    same = (row // rows == col // slot) & (place >= 0) & (place < factors)
    same &= row % rows // MEMBER_TOKENS == place // RANK
    k = lax.broadcasted_iota(jnp.int32, (2 * slot, LANES), 0)
    c = lax.broadcasted_iota(jnp.int32, (2 * slot, LANES), 1)
    pick = jnp.where(c == len(weight_hbm) * columns % LANES + k % RANK, 1.0, 0.0).astype(jnp.bfloat16)

    def source(side, j):
        return 2 * ((where_ref[0] + j) % n_hi) + (where_ref[1] if side else 1 - where_ref[1])

    loads[0].wait()
    for side in range(2):
        for j in range(n_hi):
            at = (side * n_hi + j) * block
            token_ref[at : at + rows] = near_ref[source(side, j), :rows]
            token_ref[at + rows : at + block] = near_ref[source(side, j), slot : slot + rows]
            left_ref[side * n_hi + j, 0] = near_ref[source(side, j), rows:slot]
            left_ref[side * n_hi + j, 1] = near_ref[source(side, j), slot + rows :]
            projection = dot_t(token_ref[at : at + block], near_ref[source(side, j)])
            projection = jnp.where(same, projection, 0.0).astype(jnp.bfloat16)
            tail_ref[side * n_hi + j] = jnp.dot(projection, pick, preferred_element_type=jnp.float32)
    stores = [pltpu.make_async_copy(left_ref, left_hbm, in_sems.at[0])]
    stores[0].start()
    ready = 0
    for n in range(wide // CHUNK):
        while ready < len(weight_hbm) and ready * columns < (n + 1) * CHUNK:
            part = weight_ref.at[pl.ds(ready * columns, columns)]
            pltpu.make_async_copy(weight_hbm[0], part, in_sems.at[1 + ready]).wait()
            ready += 1
        cut = pl.ds(n * CHUNK, CHUNK)
        for side, out_hbm in enumerate((sent_hbm, kept_hbm)):
            some = token_ref[side * n_hi * block : (side + 1) * n_hi * block]
            product = dot_t(some, weight_ref[cut]).reshape(n_hi, block, CHUNK)
            if (n + 1) * CHUNK < wide:
                out_ref[side, :, :, cut] = product.astype(out_ref.dtype)
            else:
                last = pl.ds(n * CHUNK + CHUNK - LANES, LANES)
                tails = tail_ref[side * n_hi : (side + 1) * n_hi]
                out_ref[side, :, :, pl.ds(n * CHUNK, CHUNK - LANES)] = product[..., :-LANES].astype(out_ref.dtype)
                out_ref[side, :, :, last] = (product[..., -LANES:] + tails).astype(out_ref.dtype)
            store = pltpu.make_async_copy(out_ref.at[side, :, :, cut], out_hbm.at[:, :, cut], out_sems.at[side, n])
            store.start()
            stores.append(store)
    for store in stores:
        store.wait()


def partials(near, weights, where, rows, factors):
    n_hi = 4
    columns, features = weights[0].shape
    wide = -(-(len(weights) * columns + RANK) // CHUNK) * CHUNK
    blocks = near.reshape(2 * n_hi, -1, features)
    block = 2 * rows
    slot = blocks.shape[1] // 2
    anywhere = pl.BlockSpec(memory_space=pl.ANY)
    half = jax.ShapeDtypeStruct((n_hi, block, wide), jnp.bfloat16)
    return pl.pallas_call(
        functools.partial(partial_kernel, rows, factors),
        in_specs=[pl.BlockSpec(memory_space=pltpu.SMEM)] + [anywhere] * (1 + len(weights)),
        out_specs=[anywhere] * 3,
        out_shape=[half, half, jax.ShapeDtypeStruct((2 * n_hi, 2, slot - rows, features), jnp.bfloat16)],
        scratch_shapes=[
            pltpu.VMEM(blocks.shape, jnp.bfloat16),
            pltpu.VMEM((wide, features), jnp.bfloat16),
            pltpu.VMEM((2 * n_hi * block, features), jnp.bfloat16),
            pltpu.VMEM((2 * n_hi, 2, slot - rows, features), jnp.bfloat16),
            pltpu.VMEM((2 * n_hi, block, LANES), jnp.float32),
            pltpu.VMEM((2, n_hi, block, wide), jnp.bfloat16),
            pltpu.SemaphoreType.DMA((1 + len(weights),)),
            pltpu.SemaphoreType.DMA((2, wide // CHUNK)),
        ],
        cost_estimate=pl.CostEstimate(
            flops=4 * n_hi * block * wide * features,
            transcendentals=0,
            bytes_accessed=2 * (wide * features + blocks.size + 2 * n_hi * block * wide),
        ),
    )(where, blocks, *weights)


def body(tokens, up_weight, left_factors, right_factors, fitness):
    f32, bf16 = jnp.float32, jnp.bfloat16
    hi, core, x = lax.axis_index("hi"), lax.axis_index("core"), lax.axis_index("x")
    rows, features = tokens.shape
    factors = left_factors.shape[0]
    columns = up_weight.shape[1]
    own = right_factors.shape[0]
    n_x, n_hi, n_z, n_lo = (lax.axis_size(a) for a in ("x", "hi", "z", "lo"))

    weight = up_weight.T
    mine = jnp.concatenate([tokens, left_factors, jnp.zeros((4, features), bf16)], 0)
    near = gathered(mine, ("z", "lo"))
    weight_far = shifted(weight, "x", 2)
    weight_after = shifted(weight, "x", -1)
    weight_before = shifted(weight, "x", 1)
    right_far = shifted(right_factors, "hi", 2)
    right_after = shifted(right_factors, "hi", -1)
    right_before = shifted(right_factors, "hi", 1)
    right_same = jnp.stack([right_factors, right_after, right_far, right_before])
    right_other = shifted(right_same, "core", 1)

    block = n_lo * rows
    weights = (weight, weight_after, weight_far, weight_before)
    sent, kept, near_left = partials(near, weights, jnp.stack([hi, core, x]), rows, factors)
    other = shifted(sent, "core", 1)

    def both(j, start, stop, parts):
        return parts[0][j, start:stop].astype(f32) + parts[1][j, start:stop].astype(f32)

    halves = kept, other
    later = lax.optimization_barrier(halves)
    cut = block // 2
    far_after = shifted(both(2, 0, cut, halves).astype(bf16), "hi", 1)
    far_before = shifted(both(2, cut, block, halves).astype(bf16), "hi", -1)
    high_before, low_after = both(1, cut, block, later).astype(bf16), both(3, 0, cut, later).astype(bf16)
    high_before = shifted(high_before, "hi", 1)
    low_after = shifted(low_after, "hi", -1)
    low_before = shifted((both(1, 0, cut, halves) + far_after.astype(f32)).astype(bf16), "hi", 1)
    high_after = shifted((both(3, cut, block, halves) + far_before.astype(f32)).astype(bf16), "hi", -1)
    kept, other, *received = lax.optimization_barrier((kept, other, low_before, low_after, high_before, high_after))
    low_before, low_after, high_before, high_after = received
    halves = kept, other
    low = both(0, 0, cut, halves) + low_before.astype(f32) + low_after.astype(f32)
    high = both(0, cut, block, halves) + high_before.astype(f32) + high_after.astype(f32)
    total = jnp.concatenate([low, high], 0).astype(bf16)

    tail = total[:, n_x * columns : n_x * columns + RANK]
    pieces = [jnp.concatenate([total[:, j * columns : (j + 1) * columns], tail], 1) for j in range(n_x)]
    whole = lax.all_to_all(jnp.stack(pieces), "x", split_axis=0, concat_axis=0, tiled=True)
    whole = whole.reshape(n_x * block, columns + RANK)
    tiled = jnp.tile(whole[:, columns:], (1, own // RANK))
    of_member = np.arange(n_x * block)[:, None] // MEMBER_TOKENS == np.arange(own) // RANK
    spread = tiled * jnp.asarray(of_member, bf16)
    correction = jnp.dot(spread, right_factors, preferred_element_type=f32)
    hidden = (whole[:, :columns].astype(f32) + MIXING * correction).astype(bf16)

    turn, z_core = jnp.arange(2 * n_hi) % n_hi, jnp.arange(2 * n_hi) // n_hi
    z = 2 * ((hi + turn) % n_hi) + jnp.where(z_core == 1, core, 1 - core)
    member = ((z[:, None] * n_x + x) * n_lo + jnp.arange(n_lo)) * (rows // MEMBER_TOKENS)
    member = member[:, :, None] + jnp.arange(factors) // RANK
    fit = jnp.sum(jnp.where(member[..., None] == jnp.arange(fitness.shape[0]), fitness, 0.0), -1)
    weighted = (fit[..., None] * near_left[:, :, :factors].astype(f32)).astype(bf16).reshape(-1, features)
    lefts = gathered(weighted, "x")
    lefts = lefts.reshape(n_x, n_z, n_lo * factors, features).transpose(1, 0, 2, 3).reshape(-1, features)
    rights = jnp.concatenate([right_other, right_same], 0).reshape(-1, columns)
    gradient = jnp.einsum("kd,kf->df", lefts, rights, preferred_element_type=f32)
    return hidden, (gradient * GRADIENT_SCALE).astype(bf16)


def solution(mesh):
    finer = Mesh(mesh.devices.reshape(8, 4, 2, 4, 2), MEMBER + TENSOR)
    return jax.shard_map(
        body,
        mesh=finer,
        in_specs=(P(MEMBER, TENSOR), P(TENSOR, MEMBER), P(MEMBER, TENSOR), P(TENSOR, MEMBER), P()),
        out_specs=(P(TENSOR, MEMBER), P(TENSOR, MEMBER)),
        check_vma=False,
    )
```

```python
import functools

import jax
import jax.numpy as jnp
import numpy as np
from jax import lax
from jax.experimental import pallas as pl
from jax.experimental.pallas import tpu as pltpu
from jax.sharding import Mesh
from jax.sharding import PartitionSpec as P


D = 5120
RANK = 4
MEMBER_TOKENS = 16
POPULATION = 192
MEMBER = ("z", "x", "lo")
TENSOR = ("hi", "core")
SIGMA = 0.25 * D**-0.5
MIXING = SIGMA * RANK**-0.5
GRADIENT_SCALE = 1.0 / (POPULATION * SIGMA * RANK**0.5)


def shifted(array, axis, step):
    size = lax.axis_size(axis)
    return lax.ppermute(array, axis, [(k, (k + step) % size) for k in range(size)])


def gathered(array, axes):
    copies = jnp.broadcast_to(array, (lax.axis_size(axes), *array.shape))
    return lax.all_to_all(copies, axes, split_axis=0, concat_axis=0, tiled=True)


def dot_t(a, b):
    return lax.dot_general(a, b, (((1,), (1,)), ((), ())), preferred_element_type=jnp.float32)


CHUNK = 256
LANES = 128
SLOTS = ((2, 0), (1, 1), (2, 1), (3, 0), (1, 0), (3, 1), (0, 0), (0, 1))


def partial_kernel(rows, where_ref, near_hbm, *refs):
    *weight_hbm, sent_hbm, kept_hbm, left_hbm, near_ref, weight_ref, token_ref, factor_ref, left_ref, tail_ref, out_ref, in_sems, out_sems = refs
    slot = near_ref.shape[1] // 2
    n_slots = len(SLOTS)
    n_hi = n_slots // 2
    wide, features = weight_ref.shape
    columns = weight_hbm[0].shape[0]
    loads = [pltpu.make_async_copy(near_hbm, near_ref, in_sems.at[0])]
    for j, some in enumerate(weight_hbm):
        place = lax.rem(where_ref[2] + j, len(weight_hbm))
        part = weight_ref.at[pl.ds(pl.multiple_of(place * columns, 16), columns)]
        loads.append(pltpu.make_async_copy(some, part, in_sems.at[1 + place]))
    for load in loads:
        load.start()
    weight_ref[len(weight_hbm) * columns :] = jnp.zeros((wide - len(weight_hbm) * columns, features), jnp.bfloat16)
    factor_rows = slot - rows
    wide_factors = n_slots * factor_rows
    pair = (n_slots, rows, wide_factors)
    token_slot, token, place = (lax.broadcasted_iota(jnp.int32, pair, d) for d in range(3))
    same = (token_slot == place // factor_rows) & (token // MEMBER_TOKENS == place % factor_rows // RANK)
    k = lax.broadcasted_iota(jnp.int32, (wide_factors, LANES), 0)
    c = lax.broadcasted_iota(jnp.int32, (wide_factors, LANES), 1)
    pick = jnp.where(c == len(weight_hbm) * columns % LANES + k % RANK, 1.0, 0.0).astype(jnp.bfloat16)
    loads[0].wait()
    for side in range(2):
        for j in range(n_hi):
            source = 2 * ((where_ref[0] + j) % n_hi) + (where_ref[1] if side else 1 - where_ref[1])
            for half in range(2):
                mine = side * n_slots + SLOTS.index((j, half))
                own = near_ref[source, half * slot : (half + 1) * slot]
                token_ref[mine * rows : (mine + 1) * rows] = own[:rows]
                factor_ref[mine * factor_rows : (mine + 1) * factor_rows] = own[rows:]
                left_ref[side * n_hi + j, half] = own[rows:]
        some = token_ref[side * n_slots * rows : (side + 1) * n_slots * rows]
        projection = dot_t(some, factor_ref[side * wide_factors : (side + 1) * wide_factors])
        projection = jnp.where(same, projection.reshape(pair), 0.0).reshape(projection.shape).astype(jnp.bfloat16)
        tail = jnp.dot(projection, pick, preferred_element_type=jnp.float32)
        tail_ref[side * n_slots : (side + 1) * n_slots] = tail.reshape(n_slots, rows, LANES)
    stores = [pltpu.make_async_copy(left_ref, left_hbm, in_sems.at[0])]
    stores[0].start()
    ready = 0
    for n in range(wide // CHUNK):
        while ready < len(weight_hbm) and ready * columns < (n + 1) * CHUNK:
            part = weight_ref.at[pl.ds(ready * columns, columns)]
            pltpu.make_async_copy(weight_hbm[0], part, in_sems.at[1 + ready]).wait()
            ready += 1
        cut = pl.ds(n * CHUNK, CHUNK)
        for side, out_hbm in enumerate((sent_hbm, kept_hbm)):
            some = token_ref[side * n_slots * rows : (side + 1) * n_slots * rows]
            product = dot_t(some, weight_ref[cut]).reshape(n_slots, rows, CHUNK)
            if (n + 1) * CHUNK < wide:
                out_ref[side, :, :, cut] = product.astype(out_ref.dtype)
            else:
                last = pl.ds(n * CHUNK + CHUNK - LANES, LANES)
                tails = tail_ref[side * n_slots : (side + 1) * n_slots]
                out_ref[side, :, :, pl.ds(n * CHUNK, CHUNK - LANES)] = product[..., :-LANES].astype(out_ref.dtype)
                out_ref[side, :, :, last] = (product[..., -LANES:] + tails).astype(out_ref.dtype)
            store = pltpu.make_async_copy(out_ref.at[side, :, :, cut], out_hbm.at[:, :, cut], out_sems.at[side, n])
            store.start()
            stores.append(store)
    for store in stores:
        store.wait()


def partials(near, weights, where, rows):
    n_hi = 4
    columns, features = weights[0].shape
    wide = -(-(len(weights) * columns + RANK) // CHUNK) * CHUNK
    blocks = near.reshape(2 * n_hi, -1, features)
    block = 2 * rows
    slot = blocks.shape[1] // 2
    anywhere = pl.BlockSpec(memory_space=pl.ANY)
    half = jax.ShapeDtypeStruct((len(SLOTS), rows, wide), jnp.bfloat16)
    return pl.pallas_call(
        functools.partial(partial_kernel, rows),
        in_specs=[pl.BlockSpec(memory_space=pltpu.SMEM)] + [anywhere] * (1 + len(weights)),
        out_specs=[anywhere] * 3,
        out_shape=[half, half, jax.ShapeDtypeStruct((2 * n_hi, 2, slot - rows, features), jnp.bfloat16)],
        scratch_shapes=[
            pltpu.VMEM(blocks.shape, jnp.bfloat16),
            pltpu.VMEM((wide, features), jnp.bfloat16),
            pltpu.VMEM((2 * n_hi * block, features), jnp.bfloat16),
            pltpu.VMEM((4 * n_hi * (slot - rows), features), jnp.bfloat16),
            pltpu.VMEM((2 * n_hi, 2, slot - rows, features), jnp.bfloat16),
            pltpu.VMEM((2 * len(SLOTS), rows, LANES), jnp.float32),
            pltpu.VMEM((2, len(SLOTS), rows, wide), jnp.bfloat16),
            pltpu.SemaphoreType.DMA((1 + len(weights),)),
            pltpu.SemaphoreType.DMA((2, wide // CHUNK)),
        ],
        cost_estimate=pl.CostEstimate(
            flops=4 * n_hi * block * wide * features,
            transcendentals=0,
            bytes_accessed=2 * (wide * features + blocks.size + 2 * n_hi * block * wide),
        ),
    )(where, blocks, *weights)


def body(tokens, up_weight, left_factors, right_factors, fitness):
    f32, bf16 = jnp.float32, jnp.bfloat16
    hi, core, x = lax.axis_index("hi"), lax.axis_index("core"), lax.axis_index("x")
    rows, features = tokens.shape
    factors = left_factors.shape[0]
    columns = up_weight.shape[1]
    own = right_factors.shape[0]
    n_x, n_hi, _, n_lo = (lax.axis_size(a) for a in ("x", "hi", "z", "lo"))

    weight = up_weight.T
    mine = jnp.concatenate([tokens, left_factors, jnp.zeros((4, features), bf16)], 0)
    near = gathered(mine, ("z", "lo"))
    weight_far = shifted(weight, "x", 2)
    weight_after = shifted(weight, "x", -1)
    weight_before = shifted(weight, "x", 1)
    right_far = shifted(right_factors, "hi", 2)
    right_after = shifted(right_factors, "hi", -1)
    right_before = shifted(right_factors, "hi", 1)
    right_same = jnp.stack([right_factors, right_after, right_far, right_before])
    right_other = shifted(right_same, "core", 1)

    block = n_lo * rows
    weights = (weight, weight_after, weight_far, weight_before)
    sent, kept, near_left = partials(near, weights, jnp.stack([hi, core, x]), rows)
    other = shifted(sent, "core", 1)

    def both(start, stop, parts):
        return parts[0][start:stop].astype(f32) + parts[1][start:stop].astype(f32)

    halves = kept, other
    up = shifted(both(0, 2, halves).astype(bf16), "hi", 1)
    down = both(2, 4, lax.optimization_barrier(halves)).astype(bf16)
    down = shifted(down, "hi", -1)
    low = shifted((both(4, 5, halves)[0] + up[0].astype(f32)).astype(bf16), "hi", 1)
    halves = lax.optimization_barrier(halves)
    high = shifted((both(5, 6, halves)[0] + down[0].astype(f32)).astype(bf16), "hi", -1)
    *halves, up, down, low, high = lax.optimization_barrier((*halves[:2], up, down, low, high))
    own_blocks = both(6, 8, halves)
    low = own_blocks[0] + low.astype(f32) + down[1].astype(f32)
    high = own_blocks[1] + high.astype(f32) + up[1].astype(f32)
    total = jnp.concatenate([low, high], 0).astype(bf16)

    tail = total[:, n_x * columns : n_x * columns + RANK]
    pieces = [jnp.concatenate([total[:, j * columns : (j + 1) * columns], tail], 1) for j in range(n_x)]
    whole = lax.all_to_all(jnp.stack(pieces), "x", split_axis=0, concat_axis=0, tiled=True)
    whole = whole.reshape(n_x * block, columns + RANK)
    tiled = jnp.tile(whole[:, columns:], (1, own // RANK))
    of_member = np.arange(n_x * block)[:, None] // MEMBER_TOKENS == np.arange(own) // RANK
    spread = tiled * jnp.asarray(of_member, bf16)
    correction = jnp.dot(spread, right_factors, preferred_element_type=f32)
    hidden = (whole[:, :columns].astype(f32) + MIXING * correction).astype(bf16)

    turn, z_core = jnp.arange(2 * n_hi) % n_hi, jnp.arange(2 * n_hi) // n_hi
    z = 2 * ((hi + turn) % n_hi) + jnp.where(z_core == 1, core, 1 - core)
    member = ((z[:, None] * n_x + x) * n_lo + jnp.arange(n_lo)) * (rows // MEMBER_TOKENS)
    member = member[:, :, None] + jnp.arange(factors) // RANK
    fit = jnp.sum(jnp.where(member[..., None] == jnp.arange(fitness.shape[0]), fitness, 0.0), -1)
    weighted = (fit[..., None] * near_left[:, :, :factors].astype(f32)).astype(bf16).reshape(-1, features)
    lefts = gathered(weighted, "x")
    lefts = lefts.reshape(n_x, 2, n_hi, n_lo * factors, features).transpose(1, 2, 0, 3, 4).reshape(2, -1, features)
    gradient = 0.0
    for left, right in zip(lefts, (right_other, right_same)):
        gradient += jnp.einsum("kd,kf->df", left, right.reshape(-1, columns), preferred_element_type=f32)
    return hidden, (gradient * GRADIENT_SCALE).astype(bf16)


def solution(mesh):
    finer = Mesh(mesh.devices.reshape(8, 4, 2, 4, 2), MEMBER + TENSOR)
    return jax.shard_map(
        body,
        mesh=finer,
        in_specs=(P(MEMBER, TENSOR), P(TENSOR, MEMBER), P(MEMBER, TENSOR), P(TENSOR, MEMBER), P()),
        out_specs=(P(TENSOR, MEMBER), P(TENSOR, MEMBER)),
        check_vma=False,
    )
```

```python
import functools

import jax
import jax.numpy as jnp
import numpy as np
from jax import lax
from jax.experimental import pallas as pl
from jax.experimental.pallas import tpu as pltpu
from jax.sharding import Mesh
from jax.sharding import PartitionSpec as P


D = 5120
RANK = 4
MEMBER_TOKENS = 16
POPULATION = 192
MEMBER = ("z", "x", "lo")
TENSOR = ("hi", "core")
SIGMA = 0.25 * D**-0.5
MIXING = SIGMA * RANK**-0.5
GRADIENT_SCALE = 1.0 / (POPULATION * SIGMA * RANK**0.5)


def shifted(array, axis, step):
    size = lax.axis_size(axis)
    return lax.ppermute(array, axis, [(k, (k + step) % size) for k in range(size)])


def gathered(array, axes):
    copies = jnp.broadcast_to(array, (lax.axis_size(axes), *array.shape))
    return lax.all_to_all(copies, axes, split_axis=0, concat_axis=0, tiled=True)


def dot_t(a, b):
    return lax.dot_general(a, b, (((1,), (1,)), ((), ())), preferred_element_type=jnp.float32)


LANES = 128


def partial_kernel(rows, where_ref, near_hbm, *refs):
    *weight_hbm, sent_hbm, kept_hbm, left_hbm = refs[:-9]
    near_ref, weight_ref, token_ref, factor_ref, left_ref, tail_ref, out_ref, in_sems, out_sems = refs[-9:]
    slot = near_ref.shape[1] // 2
    factor_rows = slot - rows
    n_x, wide, features = weight_ref.shape
    n_hi = out_ref.shape[1]
    columns = weight_hbm[0].shape[0]
    loads = [pltpu.make_async_copy(near_hbm, near_ref, in_sems.at[0])]
    for j, some in enumerate(weight_hbm):
        place = lax.rem(where_ref[2] + j, n_x)
        loads.append(pltpu.make_async_copy(some, weight_ref.at[place, pl.ds(0, columns)], in_sems.at[1 + place]))
    for load in loads:
        load.start()
    weight_ref[:, columns:] = jnp.zeros((n_x, wide - columns, features), jnp.bfloat16)
    n_slots = 2 * n_hi
    wide_factors = n_slots * factor_rows
    pair = (n_slots, rows, wide_factors)
    token_slot, token, place = (lax.broadcasted_iota(jnp.int32, pair, d) for d in range(3))
    same = (token_slot == place // factor_rows) & (token // MEMBER_TOKENS == place % factor_rows // RANK)
    k = lax.broadcasted_iota(jnp.int32, (wide_factors, LANES), 0)
    c = lax.broadcasted_iota(jnp.int32, (wide_factors, LANES), 1)
    pick = jnp.where(c == columns % LANES + k % RANK, 1.0, 0.0).astype(jnp.bfloat16)
    loads[0].wait()
    for side in range(2):
        core = where_ref[1] if side else 1 - where_ref[1]
        for j in range(n_hi):
            turned = 2 * ((where_ref[0] + j) % n_hi) + core
            for half in range(2):
                left_ref[side * n_hi + j, half] = near_ref[turned, half * slot + rows : (half + 1) * slot]
                mine = (side * n_hi + j) * 2 + half
                own = near_ref[2 * j + core, half * slot : (half + 1) * slot]
                token_ref[mine * rows : (mine + 1) * rows] = own[:rows]
                factor_ref[mine * factor_rows : (mine + 1) * factor_rows] = own[rows:]
        some = token_ref[side * n_slots * rows : (side + 1) * n_slots * rows]
        projection = dot_t(some, factor_ref[side * wide_factors : (side + 1) * wide_factors])
        projection = jnp.where(same, projection.reshape(pair), 0.0).reshape(projection.shape).astype(jnp.bfloat16)
        tail_ref[side] = jnp.dot(projection, pick, preferred_element_type=jnp.float32)
    stores = [pltpu.make_async_copy(left_ref, left_hbm, in_sems.at[0])]
    stores[0].start()
    spot = columns // LANES * LANES
    for n in range(n_x):
        part = weight_ref.at[n, pl.ds(0, columns)]
        pltpu.make_async_copy(weight_hbm[0], part, in_sems.at[1 + n]).wait()
        for side, out_hbm in enumerate((sent_hbm, kept_hbm)):
            some = token_ref[side * n_slots * rows : (side + 1) * n_slots * rows]
            product = dot_t(some, weight_ref[n])
            last = product[:, spot:] + tail_ref[side]
            out_ref[side, :, n, :, :spot] = product[:, :spot].reshape(n_hi, 2 * rows, spot).astype(out_ref.dtype)
            out_ref[side, :, n, :, spot:] = last.reshape(n_hi, 2 * rows, LANES).astype(out_ref.dtype)
            store = pltpu.make_async_copy(out_ref.at[side, :, n], out_hbm.at[:, n], out_sems.at[side, n])
            store.start()
            stores.append(store)
    for store in stores:
        store.wait()


def partials(near, weights, where, rows):
    n_hi, n_x = 4, len(weights)
    columns, features = weights[0].shape
    wide = -(-(columns + RANK) // LANES) * LANES
    blocks = near.reshape(2 * n_hi, -1, features)
    block = 2 * rows
    slot = blocks.shape[1] // 2
    anywhere = pl.BlockSpec(memory_space=pl.ANY)
    half = jax.ShapeDtypeStruct((n_hi, n_x, block, wide), jnp.bfloat16)
    return pl.pallas_call(
        functools.partial(partial_kernel, rows),
        in_specs=[pl.BlockSpec(memory_space=pltpu.SMEM)] + [anywhere] * (1 + n_x),
        out_specs=[anywhere] * 3,
        out_shape=[half, half, jax.ShapeDtypeStruct((2 * n_hi, 2, slot - rows, features), jnp.bfloat16)],
        scratch_shapes=[
            pltpu.VMEM(blocks.shape, jnp.bfloat16),
            pltpu.VMEM((n_x, wide, features), jnp.bfloat16),
            pltpu.VMEM((2 * n_hi * block, features), jnp.bfloat16),
            pltpu.VMEM((4 * n_hi * (slot - rows), features), jnp.bfloat16),
            pltpu.VMEM((2 * n_hi, 2, slot - rows, features), jnp.bfloat16),
            pltpu.VMEM((2, n_hi * block, LANES), jnp.float32),
            pltpu.VMEM((2, *half.shape), jnp.bfloat16),
            pltpu.SemaphoreType.DMA((1 + n_x,)),
            pltpu.SemaphoreType.DMA((2, n_x)),
        ],
        cost_estimate=pl.CostEstimate(
            flops=4 * n_hi * block * n_x * wide * features,
            transcendentals=0,
            bytes_accessed=2 * (n_x * wide * features + blocks.size + 2 * n_hi * block * n_x * wide),
        ),
    )(where, blocks, *weights)


def body(tokens, up_weight, left_factors, right_factors, fitness):
    f32, bf16 = jnp.float32, jnp.bfloat16
    hi, core, x = lax.axis_index("hi"), lax.axis_index("core"), lax.axis_index("x")
    rows, features = tokens.shape
    factors = left_factors.shape[0]
    columns = up_weight.shape[1]
    own = right_factors.shape[0]
    n_x, n_hi, _, n_lo = (lax.axis_size(a) for a in ("x", "hi", "z", "lo"))

    weight = up_weight.T
    mine = jnp.concatenate([tokens, left_factors, jnp.zeros((4, features), bf16)], 0)
    near = gathered(mine, ("z", "lo"))
    weight_far = shifted(weight, "x", 2)
    weight_after = shifted(weight, "x", -1)
    weight_before = shifted(weight, "x", 1)
    right_far = shifted(right_factors, "hi", 2)
    right_after = shifted(right_factors, "hi", -1)
    right_before = shifted(right_factors, "hi", 1)
    right_same = jnp.stack([right_factors, right_after, right_far, right_before])
    right_other = shifted(right_same, "core", 1)

    block = n_lo * rows
    weights = (weight, weight_after, weight_far, weight_before)
    sent, kept, near_left = partials(near, weights, jnp.stack([hi, core, x]), rows)
    other = shifted(sent, "core", 1)

    both = (kept.astype(f32) + other.astype(f32)).astype(bf16).reshape(n_hi * n_x, block, -1)

    whole = lax.all_to_all(both, ("hi", "x"), split_axis=0, concat_axis=0, tiled=True)
    whole = jnp.sum(whole.reshape(n_hi, n_x * block, -1).astype(f32), 0)
    tiled = jnp.tile(whole[:, columns : columns + RANK].astype(bf16), (1, own // RANK))
    of_member = np.arange(n_x * block)[:, None] // MEMBER_TOKENS == np.arange(own) // RANK
    spread = tiled * jnp.asarray(of_member, bf16)
    correction = jnp.dot(spread, right_factors, preferred_element_type=f32)
    hidden = (whole[:, :columns] + MIXING * correction).astype(bf16)

    turn, z_core = jnp.arange(2 * n_hi) % n_hi, jnp.arange(2 * n_hi) // n_hi
    z = 2 * ((hi + turn) % n_hi) + jnp.where(z_core == 1, core, 1 - core)
    member = ((z[:, None] * n_x + x) * n_lo + jnp.arange(n_lo)) * (rows // MEMBER_TOKENS)
    member = member[:, :, None] + jnp.arange(factors) // RANK
    fit = jnp.sum(jnp.where(member[..., None] == jnp.arange(fitness.shape[0]), fitness, 0.0), -1)
    weighted = (fit[..., None] * near_left[:, :, :factors].astype(f32)).astype(bf16).reshape(-1, features)
    lefts = [weighted] + [shifted(weighted, "x", -j) for j in range(1, n_x)]
    lefts = jnp.stack(lefts + lefts[:-1])
    lefts = lax.dynamic_slice_in_dim(lefts, (n_x - x) % n_x, n_x)
    lefts = lefts.reshape(n_x, 2, n_hi, n_lo * factors, features).transpose(1, 2, 0, 3, 4).reshape(2, -1, features)
    gradient = 0.0
    for left, right in zip(lefts, (right_other, right_same)):
        gradient += jnp.einsum("kd,kf->df", left, right.reshape(-1, columns), preferred_element_type=f32)
    return hidden, (gradient * GRADIENT_SCALE).astype(bf16)


def solution(mesh):
    finer = Mesh(mesh.devices.reshape(8, 4, 2, 4, 2), MEMBER + TENSOR)
    return jax.shard_map(
        body,
        mesh=finer,
        in_specs=(P(MEMBER, TENSOR), P(TENSOR, MEMBER), P(MEMBER, TENSOR), P(TENSOR, MEMBER), P()),
        out_specs=(P(TENSOR, MEMBER), P(TENSOR, MEMBER)),
        check_vma=False,
    )
```

```python
import functools

import jax
import jax.numpy as jnp
import numpy as np
from jax import lax
from jax.experimental import pallas as pl
from jax.experimental.pallas import tpu as pltpu
from jax.sharding import Mesh
from jax.sharding import PartitionSpec as P


D = 5120
RANK = 4
MEMBER_TOKENS = 16
POPULATION = 192
MEMBER = ("z", "x", "lo")
TENSOR = ("hi", "core")
SIGMA = 0.25 * D**-0.5
MIXING = SIGMA * RANK**-0.5
GRADIENT_SCALE = 1.0 / (POPULATION * SIGMA * RANK**0.5)


def shifted(array, axis, step):
    size = lax.axis_size(axis)
    return lax.ppermute(array, axis, [(k, (k + step) % size) for k in range(size)])


def gathered(array, axes):
    copies = jnp.broadcast_to(array, (lax.axis_size(axes), *array.shape))
    return lax.all_to_all(copies, axes, split_axis=0, concat_axis=0, tiled=True)


def dot_t(a, b):
    return lax.dot_general(a, b, (((1,), (1,)), ((), ())), preferred_element_type=jnp.float32)


LANES = 128


def partial_kernel(rows, where_ref, near_hbm, *refs):
    *weight_hbm, sent_hbm, kept_hbm, left_hbm = refs[:-9]
    near_ref, weight_ref, token_ref, factor_ref, left_ref, tail_ref, out_ref, in_sems, out_sems = refs[-9:]
    slot = near_ref.shape[1] // 2
    factor_rows = slot - rows
    n_x, wide, features = weight_ref.shape
    n_hi = out_ref.shape[1]
    columns = weight_hbm[0].shape[0]
    loads = [pltpu.make_async_copy(near_hbm, near_ref, in_sems.at[0])]
    for j, some in enumerate(weight_hbm):
        place = lax.rem(where_ref[2] + j, n_x)
        loads.append(pltpu.make_async_copy(some, weight_ref.at[place, pl.ds(0, columns)], in_sems.at[1 + place]))
    for load in loads:
        load.start()
    weight_ref[:, columns:] = jnp.zeros((n_x, wide - columns, features), jnp.bfloat16)
    n_slots = 2 * n_hi
    wide_factors = n_slots * factor_rows
    pair = (n_slots, rows, wide_factors)
    token_slot, token, place = (lax.broadcasted_iota(jnp.int32, pair, d) for d in range(3))
    same = (token_slot == place // factor_rows) & (token // MEMBER_TOKENS == place % factor_rows // RANK)
    k = lax.broadcasted_iota(jnp.int32, (wide_factors, LANES), 0)
    c = lax.broadcasted_iota(jnp.int32, (wide_factors, LANES), 1)
    pick = jnp.where(c == columns % LANES + k % RANK, 1.0, 0.0).astype(jnp.bfloat16)
    loads[0].wait()
    for side in range(2):
        core = where_ref[1] if side else 1 - where_ref[1]
        for j in range(n_hi):
            turned = 2 * ((where_ref[0] + j) % n_hi) + core
            for half in range(2):
                left_ref[side * n_hi + j, half] = near_ref[turned, half * slot + rows : (half + 1) * slot]
                mine = (side * n_hi + j) * 2 + half
                own = near_ref[2 * j + core, half * slot : (half + 1) * slot]
                token_ref[mine * rows : (mine + 1) * rows] = own[:rows]
                factor_ref[mine * factor_rows : (mine + 1) * factor_rows] = own[rows:]
        some = token_ref[side * n_slots * rows : (side + 1) * n_slots * rows]
        projection = dot_t(some, factor_ref[side * wide_factors : (side + 1) * wide_factors])
        projection = jnp.where(same, projection.reshape(pair), 0.0).reshape(projection.shape).astype(jnp.bfloat16)
        tail_ref[side] = jnp.dot(projection, pick, preferred_element_type=jnp.float32)
    stores = [pltpu.make_async_copy(left_ref, left_hbm, in_sems.at[0])]
    stores[0].start()
    spot = columns // LANES * LANES
    for n in range(n_x):
        part = weight_ref.at[n, pl.ds(0, columns)]
        pltpu.make_async_copy(weight_hbm[0], part, in_sems.at[1 + n]).wait()
        for side, out_hbm in enumerate((sent_hbm, kept_hbm)):
            some = token_ref[side * n_slots * rows : (side + 1) * n_slots * rows]
            product = dot_t(some, weight_ref[n])
            product = product.reshape(n_hi, 2 * rows, wide)
            last = product[..., spot:] + tail_ref[side].reshape(n_hi, 2 * rows, LANES)
            for j in range(n_hi):
                for lane in range(spot // LANES):
                    piece = product[j, :, lane * LANES : (lane + 1) * LANES]
                    out_ref[side, j, n, lane * 2 * rows : (lane + 1) * 2 * rows] = piece.astype(out_ref.dtype)
                packed = last[j, :rows] + pltpu.roll(last[j, rows:], LANES // 2, 1)
                out_ref[side, j, n, spot // LANES * 2 * rows :] = packed.astype(out_ref.dtype)
            store = pltpu.make_async_copy(out_ref.at[side, :, n], out_hbm.at[:, n], out_sems.at[side, n])
            store.start()
            stores.append(store)
    for store in stores:
        store.wait()


def partials(near, weights, where, rows):
    n_hi, n_x = 4, len(weights)
    columns, features = weights[0].shape
    wide = -(-(columns + RANK) // LANES) * LANES
    blocks = near.reshape(2 * n_hi, -1, features)
    block = 2 * rows
    slot = blocks.shape[1] // 2
    anywhere = pl.BlockSpec(memory_space=pl.ANY)
    deep = columns // LANES * block + rows
    half = jax.ShapeDtypeStruct((n_hi, n_x, deep, LANES), jnp.bfloat16)
    return pl.pallas_call(
        functools.partial(partial_kernel, rows),
        in_specs=[pl.BlockSpec(memory_space=pltpu.SMEM)] + [anywhere] * (1 + n_x),
        out_specs=[anywhere] * 3,
        out_shape=[half, half, jax.ShapeDtypeStruct((2 * n_hi, 2, slot - rows, features), jnp.bfloat16)],
        scratch_shapes=[
            pltpu.VMEM(blocks.shape, jnp.bfloat16),
            pltpu.VMEM((n_x, wide, features), jnp.bfloat16),
            pltpu.VMEM((2 * n_hi * block, features), jnp.bfloat16),
            pltpu.VMEM((4 * n_hi * (slot - rows), features), jnp.bfloat16),
            pltpu.VMEM((2 * n_hi, 2, slot - rows, features), jnp.bfloat16),
            pltpu.VMEM((2, n_hi * block, LANES), jnp.float32),
            pltpu.VMEM((2, *half.shape), jnp.bfloat16),
            pltpu.SemaphoreType.DMA((1 + n_x,)),
            pltpu.SemaphoreType.DMA((2, n_x)),
        ],
        cost_estimate=pl.CostEstimate(
            flops=4 * n_hi * block * n_x * wide * features,
            transcendentals=0,
            bytes_accessed=2 * (n_x * wide * features + blocks.size + 2 * n_hi * block * n_x * wide),
        ),
    )(where, blocks, *weights)


def body(tokens, up_weight, left_factors, right_factors, fitness):
    f32, bf16 = jnp.float32, jnp.bfloat16
    hi, core, x = lax.axis_index("hi"), lax.axis_index("core"), lax.axis_index("x")
    rows, features = tokens.shape
    factors = left_factors.shape[0]
    columns = up_weight.shape[1]
    own = right_factors.shape[0]
    n_x, n_hi, _, n_lo = (lax.axis_size(a) for a in ("x", "hi", "z", "lo"))

    weight = up_weight.T
    mine = jnp.concatenate([tokens, left_factors, jnp.zeros((4, features), bf16)], 0)
    near = gathered(mine, ("z", "lo"))
    weight_far = shifted(weight, "x", 2)
    weight_after = shifted(weight, "x", -1)
    weight_before = shifted(weight, "x", 1)
    right_far = shifted(right_factors, "hi", 2)
    right_after = shifted(right_factors, "hi", -1)
    right_before = shifted(right_factors, "hi", 1)
    right_same = jnp.stack([right_factors, right_after, right_far, right_before])
    right_other = shifted(right_same, "core", 1)

    block = n_lo * rows
    weights = (weight, weight_after, weight_far, weight_before)
    sent, kept, near_left = partials(near, weights, jnp.stack([hi, core, x]), rows)
    other = shifted(sent, "core", 1)

    both = (kept.astype(f32) + other.astype(f32)).astype(bf16).reshape(n_hi * n_x, -1, LANES)

    whole = lax.all_to_all(both, ("hi", "x"), split_axis=0, concat_axis=0, tiled=True)
    whole = jnp.sum(whole.reshape(n_hi, n_x, -1, LANES).astype(f32), 0)
    tiles = columns // LANES
    main = whole[:, : tiles * block].reshape(n_x, tiles, block, LANES).transpose(0, 2, 1, 3)
    rest = whole[:, tiles * block :].reshape(n_x, rows, 2, LANES // 2).transpose(0, 2, 1, 3)
    main, rest = main.reshape(n_x * block, -1), rest.reshape(n_x * block, -1)
    over = columns % LANES
    tiled = jnp.tile(rest[:, over : over + RANK].astype(bf16), (1, own // RANK))
    of_member = np.arange(n_x * block)[:, None] // MEMBER_TOKENS == np.arange(own) // RANK
    spread = tiled * jnp.asarray(of_member, bf16)
    correction = jnp.dot(spread, right_factors, preferred_element_type=f32)
    hidden = (jnp.concatenate([main, rest[:, :over]], 1) + MIXING * correction).astype(bf16)

    turn, z_core = jnp.arange(2 * n_hi) % n_hi, jnp.arange(2 * n_hi) // n_hi
    z = 2 * ((hi + turn) % n_hi) + jnp.where(z_core == 1, core, 1 - core)
    member = ((z[:, None] * n_x + x) * n_lo + jnp.arange(n_lo)) * (rows // MEMBER_TOKENS)
    member = member[:, :, None] + jnp.arange(factors) // RANK
    fit = jnp.sum(jnp.where(member[..., None] == jnp.arange(fitness.shape[0]), fitness, 0.0), -1)
    weighted = (fit[..., None] * near_left[:, :, :factors].astype(f32)).astype(bf16).reshape(-1, features)
    lefts = [weighted] + [shifted(weighted, "x", -j) for j in range(1, n_x)]
    lefts = jnp.stack(lefts + lefts[:-1])
    lefts = lax.dynamic_slice_in_dim(lefts, (n_x - x) % n_x, n_x)
    lefts = lefts.reshape(n_x, 2, n_hi, n_lo * factors, features).transpose(1, 2, 0, 3, 4).reshape(2, -1, features)
    gradient = 0.0
    for left, right in zip(lefts, (right_other, right_same)):
        gradient += jnp.einsum("kd,kf->df", left, right.reshape(-1, columns), preferred_element_type=f32)
    return hidden, (gradient * GRADIENT_SCALE).astype(bf16)


def solution(mesh):
    finer = Mesh(mesh.devices.reshape(8, 4, 2, 4, 2), MEMBER + TENSOR)
    return jax.shard_map(
        body,
        mesh=finer,
        in_specs=(P(MEMBER, TENSOR), P(TENSOR, MEMBER), P(MEMBER, TENSOR), P(TENSOR, MEMBER), P()),
        out_specs=(P(TENSOR, MEMBER), P(TENSOR, MEMBER)),
        check_vma=False,
    )
```

```python
import functools

import jax
import jax.numpy as jnp
import numpy as np
from jax import lax
from jax.experimental import pallas as pl
from jax.experimental.pallas import tpu as pltpu
from jax.sharding import Mesh
from jax.sharding import PartitionSpec as P


D = 5120
RANK = 4
MEMBER_TOKENS = 16
POPULATION = 192
MEMBER = ("z", "x", "lo")
TENSOR = ("hi", "core")
SIGMA = 0.25 * D**-0.5
MIXING = SIGMA * RANK**-0.5
GRADIENT_SCALE = 1.0 / (POPULATION * SIGMA * RANK**0.5)


def shifted(array, axis, step):
    size = lax.axis_size(axis)
    return lax.ppermute(array, axis, [(k, (k + step) % size) for k in range(size)])


def gathered(array, axes):
    copies = jnp.broadcast_to(array, (lax.axis_size(axes), *array.shape))
    return lax.all_to_all(copies, axes, split_axis=0, concat_axis=0, tiled=True)


def dot_t(a, b):
    return lax.dot_general(a, b, (((1,), (1,)), ((), ())), preferred_element_type=jnp.float32)


LANES = 128


def partial_kernel(rows, where_ref, near_ref, *refs):
    *weight_refs, sent_ref, kept_ref, left_ref = refs[:-3]
    token_ref, factor_ref, tail_ref = refs[-3:]
    slot = near_ref.shape[1] // 2
    factor_rows = slot - rows
    n_x = len(weight_refs)
    columns, _ = weight_refs[0].shape
    n_hi = sent_ref.shape[0]
    n_slots = 2 * n_hi
    wide_factors = n_slots * factor_rows
    pair = (n_slots, rows, wide_factors)
    token_slot, token, place = (lax.broadcasted_iota(jnp.int32, pair, d) for d in range(3))
    same = (token_slot == place // factor_rows) & (token // MEMBER_TOKENS == place % factor_rows // RANK)
    k = lax.broadcasted_iota(jnp.int32, (wide_factors, LANES), 0)
    c = lax.broadcasted_iota(jnp.int32, (wide_factors, LANES), 1)
    pick = jnp.where(c == columns % LANES + k % RANK, 1.0, 0.0).astype(jnp.bfloat16)
    for side in range(2):
        core = where_ref[1] if side else 1 - where_ref[1]
        for j in range(n_hi):
            turned = 2 * ((where_ref[0] + j) % n_hi) + core
            for half in range(2):
                left_ref[side * n_hi + j, half] = near_ref[turned, half * slot + rows : (half + 1) * slot]
                mine = (side * n_hi + j) * 2 + half
                own = near_ref[2 * j + core, half * slot : (half + 1) * slot]
                token_ref[mine * rows : (mine + 1) * rows] = own[:rows]
                factor_ref[mine * factor_rows : (mine + 1) * factor_rows] = own[rows:]
        some = token_ref[side * n_slots * rows : (side + 1) * n_slots * rows]
        projection = dot_t(some, factor_ref[side * wide_factors : (side + 1) * wide_factors])
        projection = jnp.where(same, projection.reshape(pair), 0.0).reshape(projection.shape).astype(jnp.bfloat16)
        tail_ref[side] = jnp.dot(projection, pick, preferred_element_type=jnp.float32)
    spot = columns // LANES * LANES
    blank = jnp.zeros((n_hi, 2 * rows, LANES - columns % LANES), jnp.float32)
    for n, weight_ref in enumerate(weight_refs):
        place = lax.rem(where_ref[2] + n, n_x)
        for side, out_ref in enumerate((sent_ref, kept_ref)):
            some = token_ref[side * n_slots * rows : (side + 1) * n_slots * rows]
            product = dot_t(some, weight_ref[...]).reshape(n_hi, 2 * rows, columns)
            last = jnp.concatenate([product[..., spot:], blank], -1)
            last += tail_ref[side].reshape(n_hi, 2 * rows, LANES)
            for j in range(n_hi):
                for lane in range(spot // LANES):
                    piece = product[j, :, lane * LANES : (lane + 1) * LANES]
                    out_ref[j, place, lane * 2 * rows : (lane + 1) * 2 * rows] = piece.astype(out_ref.dtype)
                packed = last[j, :rows] + pltpu.roll(last[j, rows:], LANES // 2, 1)
                out_ref[j, place, spot // LANES * 2 * rows :] = packed.astype(out_ref.dtype)


def partials(near, weights, where, rows):
    n_hi, n_x = 4, len(weights)
    columns, features = weights[0].shape
    blocks = near.reshape(2 * n_hi, -1, features)
    block = 2 * rows
    slot = blocks.shape[1] // 2
    vmem = pl.BlockSpec(memory_space=pltpu.VMEM)
    half = pltpu.VMEM((n_hi, n_x, columns // LANES * block + rows, LANES), jnp.bfloat16)
    left = pltpu.VMEM((2 * n_hi, 2, slot - rows, features), jnp.bfloat16)
    return pl.pallas_call(
        functools.partial(partial_kernel, rows),
        in_specs=[pl.BlockSpec(memory_space=pltpu.SMEM)] + [vmem] * (1 + n_x),
        out_specs=[vmem] * 3,
        out_shape=[half, half, left],
        scratch_shapes=[
            pltpu.VMEM((2 * n_hi * block, features), jnp.bfloat16),
            pltpu.VMEM((4 * n_hi * (slot - rows), features), jnp.bfloat16),
            pltpu.VMEM((2, n_hi * block, LANES), jnp.float32),
        ],
        compiler_params=pltpu.CompilerParams(vmem_limit_bytes=24 * 2**20),
        cost_estimate=pl.CostEstimate(
            flops=4 * n_hi * block * n_x * columns * features,
            transcendentals=0,
            bytes_accessed=2 * (n_x * columns * features + blocks.size + 2 * n_hi * block * n_x * columns),
        ),
    )(where, *[pltpu.with_memory_space_constraint(a, pltpu.VMEM) for a in (blocks, *weights)])


def body(tokens, up_weight, left_factors, right_factors, fitness):
    f32, bf16 = jnp.float32, jnp.bfloat16
    hi, core, x = lax.axis_index("hi"), lax.axis_index("core"), lax.axis_index("x")
    rows, features = tokens.shape
    factors = left_factors.shape[0]
    columns = up_weight.shape[1]
    own = right_factors.shape[0]
    n_x, n_hi, _, n_lo = (lax.axis_size(a) for a in ("x", "hi", "z", "lo"))

    weight = up_weight.T
    mine = jnp.concatenate([tokens, left_factors, jnp.zeros((4, features), bf16)], 0)
    near = gathered(mine, ("z", "lo"))
    weight_far = shifted(weight, "x", 2)
    weight_after = shifted(weight, "x", -1)
    weight_before = shifted(weight, "x", 1)
    right_far = shifted(right_factors, "hi", 2)
    right_after = shifted(right_factors, "hi", -1)
    right_before = shifted(right_factors, "hi", 1)
    right_same = jnp.stack([right_factors, right_after, right_far, right_before])
    right_other = shifted(right_same, "core", 1)

    block = n_lo * rows
    weights = (weight, weight_after, weight_far, weight_before)
    sent, kept, near_left = partials(near, weights, jnp.stack([hi, core, x]), rows)
    other = shifted(sent, "core", 1)

    both = (kept.astype(f32) + other.astype(f32)).astype(bf16).reshape(n_hi * n_x, -1, LANES)

    whole = lax.all_to_all(both, ("hi", "x"), split_axis=0, concat_axis=0, tiled=True)
    whole = jnp.sum(whole.reshape(n_hi, n_x, -1, LANES).astype(f32), 0)
    tiles = columns // LANES
    main = whole[:, : tiles * block].reshape(n_x, tiles, block, LANES).transpose(0, 2, 1, 3)
    rest = whole[:, tiles * block :].reshape(n_x, rows, 2, LANES // 2).transpose(0, 2, 1, 3)
    main, rest = main.reshape(n_x * block, -1), rest.reshape(n_x * block, -1)
    over = columns % LANES
    tiled = jnp.tile(rest[:, over : over + RANK].astype(bf16), (1, own // RANK))
    of_member = np.arange(n_x * block)[:, None] // MEMBER_TOKENS == np.arange(own) // RANK
    spread = tiled * jnp.asarray(of_member, bf16)
    correction = jnp.dot(spread, right_factors, preferred_element_type=f32)
    hidden = (jnp.concatenate([main, rest[:, :over]], 1) + MIXING * correction).astype(bf16)

    turn, z_core = jnp.arange(2 * n_hi) % n_hi, jnp.arange(2 * n_hi) // n_hi
    z = 2 * ((hi + turn) % n_hi) + jnp.where(z_core == 1, core, 1 - core)
    member = ((z[:, None] * n_x + x) * n_lo + jnp.arange(n_lo)) * (rows // MEMBER_TOKENS)
    member = member[:, :, None] + jnp.arange(factors) // RANK
    fit = jnp.sum(jnp.where(member[..., None] == jnp.arange(fitness.shape[0]), fitness, 0.0), -1)
    weighted = (fit[..., None] * near_left[:, :, :factors].astype(f32)).astype(bf16).reshape(-1, features)
    lefts = [weighted] + [shifted(weighted, "x", -j) for j in range(1, n_x)]
    lefts = jnp.stack(lefts + lefts[:-1])
    lefts = lax.dynamic_slice_in_dim(lefts, (n_x - x) % n_x, n_x)
    lefts = lefts.reshape(n_x, 2, n_hi, n_lo * factors, features).transpose(1, 2, 0, 3, 4).reshape(2, -1, features)
    gradient = 0.0
    for left, right in zip(lefts, (right_other, right_same)):
        gradient += jnp.einsum("kd,kf->df", left, right.reshape(-1, columns), preferred_element_type=f32)
    return hidden, (gradient * GRADIENT_SCALE).astype(bf16)


def solution(mesh):
    finer = Mesh(mesh.devices.reshape(8, 4, 2, 4, 2), MEMBER + TENSOR)
    return jax.shard_map(
        body,
        mesh=finer,
        in_specs=(P(MEMBER, TENSOR), P(TENSOR, MEMBER), P(MEMBER, TENSOR), P(TENSOR, MEMBER), P()),
        out_specs=(P(TENSOR, MEMBER), P(TENSOR, MEMBER)),
        check_vma=False,
    )
```

```python
import functools

import jax
import jax.numpy as jnp
import numpy as np
from jax import lax
from jax.experimental import pallas as pl
from jax.experimental.pallas import tpu as pltpu
from jax.sharding import Mesh
from jax.sharding import PartitionSpec as P


D = 5120
RANK = 4
MEMBER_TOKENS = 16
POPULATION = 192
MEMBER = ("z", "x", "lo")
TENSOR = ("hi", "core")
SIGMA = 0.25 * D**-0.5
MIXING = SIGMA * RANK**-0.5
GRADIENT_SCALE = 1.0 / (POPULATION * SIGMA * RANK**0.5)


def shifted(array, axis, step):
    size = lax.axis_size(axis)
    return lax.ppermute(array, axis, [(k, (k + step) % size) for k in range(size)])


def gathered(array, axes):
    copies = jnp.broadcast_to(array, (lax.axis_size(axes), *array.shape))
    return lax.all_to_all(copies, axes, split_axis=0, concat_axis=0, tiled=True)


def dot_t(a, b):
    return lax.dot_general(a, b, (((1,), (1,)), ((), ())), preferred_element_type=jnp.float32)


LANES = 128


def partial_kernel(rows, where_ref, near_ref, *refs):
    *weight_refs, sent_hbm, kept_ref, left_ref = refs[:-7]
    token_ref, factor_ref, tail_ref, sent_ref, held_ref, in_sems, out_sems = refs[-7:]
    slot = near_ref.shape[1] // 2
    factor_rows = slot - rows
    n_x = len(weight_refs)
    columns, _ = weight_refs[0].shape
    n_hi = sent_ref.shape[0]
    loads = [pltpu.make_async_copy(some, held_ref.at[n], in_sems.at[n]) for n, some in enumerate(weight_refs)]
    for load in loads:
        load.start()
    n_slots = 2 * n_hi
    wide_factors = n_slots * factor_rows
    pair = (n_slots, rows, wide_factors)
    token_slot, token, place = (lax.broadcasted_iota(jnp.int32, pair, d) for d in range(3))
    same = (token_slot == place // factor_rows) & (token // MEMBER_TOKENS == place % factor_rows // RANK)
    k = lax.broadcasted_iota(jnp.int32, (wide_factors, LANES), 0)
    c = lax.broadcasted_iota(jnp.int32, (wide_factors, LANES), 1)
    pick = jnp.where(c == columns % LANES + k % RANK, 1.0, 0.0).astype(jnp.bfloat16)
    for side in range(2):
        core = where_ref[1] if side else 1 - where_ref[1]
        for j in range(n_hi):
            turned = 2 * ((where_ref[0] + j) % n_hi) + core
            for half in range(2):
                left_ref[side * n_hi + j, half] = near_ref[turned, half * slot + rows : (half + 1) * slot]
                mine = (side * n_hi + j) * 2 + half
                own = near_ref[2 * j + core, half * slot : (half + 1) * slot]
                token_ref[mine * rows : (mine + 1) * rows] = own[:rows]
                factor_ref[mine * factor_rows : (mine + 1) * factor_rows] = own[rows:]
        some = token_ref[side * n_slots * rows : (side + 1) * n_slots * rows]
        projection = dot_t(some, factor_ref[side * wide_factors : (side + 1) * wide_factors])
        projection = jnp.where(same, projection.reshape(pair), 0.0).reshape(projection.shape).astype(jnp.bfloat16)
        tail_ref[side] = jnp.dot(projection, pick, preferred_element_type=jnp.float32)
    spot = columns // LANES * LANES
    blank = jnp.zeros((n_hi, 2 * rows, LANES - columns % LANES), jnp.float32)
    stores = []
    for n in range(n_x):
        place = lax.rem(where_ref[2] + n, n_x)
        loads[n].wait()
        for side, out_ref in enumerate((sent_ref, kept_ref)):
            some = token_ref[side * n_slots * rows : (side + 1) * n_slots * rows]
            product = dot_t(some, held_ref[n]).reshape(n_hi, 2 * rows, columns)
            last = jnp.concatenate([product[..., spot:], blank], -1)
            last += tail_ref[side].reshape(n_hi, 2 * rows, LANES)
            for j in range(n_hi):
                for lane in range(spot // LANES):
                    piece = product[j, :, lane * LANES : (lane + 1) * LANES]
                    out_ref[j, place, lane * 2 * rows : (lane + 1) * 2 * rows] = piece.astype(out_ref.dtype)
                packed = last[j, :rows] + pltpu.roll(last[j, rows:], LANES // 2, 1)
                out_ref[j, place, spot // LANES * 2 * rows :] = packed.astype(out_ref.dtype)
            if side == 0:
                stores.append(pltpu.make_async_copy(sent_ref.at[:, place], sent_hbm.at[:, place], out_sems.at[n]))
                stores[-1].start()
    for store in stores:
        store.wait()


def partials(near, weights, where, rows):
    n_hi, n_x = 4, len(weights)
    columns, features = weights[0].shape
    blocks = near.reshape(2 * n_hi, -1, features)
    block = 2 * rows
    slot = blocks.shape[1] // 2
    vmem, hbm = (pl.BlockSpec(memory_space=space) for space in (pltpu.VMEM, pltpu.HBM))
    blocks = pltpu.with_memory_space_constraint(blocks, pltpu.VMEM)
    weights = [pltpu.with_memory_space_constraint(a, pltpu.HBM) for a in weights]
    half = pltpu.VMEM((n_hi, n_x, columns // LANES * block + rows, LANES), jnp.bfloat16)
    left = pltpu.VMEM((2 * n_hi, 2, slot - rows, features), jnp.bfloat16)
    return pl.pallas_call(
        functools.partial(partial_kernel, rows),
        in_specs=[pl.BlockSpec(memory_space=pltpu.SMEM), vmem] + [hbm] * n_x,
        out_specs=[hbm, vmem, vmem],
        out_shape=[jax.ShapeDtypeStruct(half.shape, half.dtype), half, left],
        scratch_shapes=[
            pltpu.VMEM((2 * n_hi * block, features), jnp.bfloat16),
            pltpu.VMEM((4 * n_hi * (slot - rows), features), jnp.bfloat16),
            pltpu.VMEM((2, n_hi * block, LANES), jnp.float32),
            half,
            pltpu.VMEM((n_x, columns, features), jnp.bfloat16),
            pltpu.SemaphoreType.DMA((n_x,)),
            pltpu.SemaphoreType.DMA((n_x,)),
        ],
        compiler_params=pltpu.CompilerParams(vmem_limit_bytes=24 * 2**20),
        cost_estimate=pl.CostEstimate(
            flops=4 * n_hi * block * n_x * columns * features,
            transcendentals=0,
            bytes_accessed=2 * (n_x * columns * features + blocks.size + 2 * n_hi * block * n_x * columns),
        ),
    )(where, blocks, *weights)


def body(tokens, up_weight, left_factors, right_factors, fitness):
    f32, bf16 = jnp.float32, jnp.bfloat16
    hi, core, x = lax.axis_index("hi"), lax.axis_index("core"), lax.axis_index("x")
    rows, features = tokens.shape
    factors = left_factors.shape[0]
    columns = up_weight.shape[1]
    own = right_factors.shape[0]
    n_x, n_hi, _, n_lo = (lax.axis_size(a) for a in ("x", "hi", "z", "lo"))

    weight = up_weight.T
    mine = jnp.concatenate([tokens, left_factors, jnp.zeros((4, features), bf16)], 0)
    near = gathered(mine, ("z", "lo"))
    weight_far = shifted(weight, "x", 2)
    weight_after = shifted(weight, "x", -1)
    weight_before = shifted(weight, "x", 1)
    right_far = shifted(right_factors, "hi", 2)
    right_after = shifted(right_factors, "hi", -1)
    right_before = shifted(right_factors, "hi", 1)
    right_same = jnp.stack([right_factors, right_after, right_far, right_before])
    right_other = shifted(right_same, "core", 1)

    block = n_lo * rows
    weights = (weight, weight_after, weight_far, weight_before)
    sent, kept, near_left = partials(near, weights, jnp.stack([hi, core, x]), rows)
    other = shifted(sent, "core", 1)

    both = (kept.astype(f32) + other.astype(f32)).astype(bf16).reshape(n_hi * n_x, -1, LANES)

    whole = lax.all_to_all(both, ("hi", "x"), split_axis=0, concat_axis=0, tiled=True)
    whole = jnp.sum(whole.reshape(n_hi, n_x, -1, LANES).astype(f32), 0)
    tiles = columns // LANES
    main = whole[:, : tiles * block].reshape(n_x, tiles, block, LANES).transpose(0, 2, 1, 3)
    rest = whole[:, tiles * block :].reshape(n_x, rows, 2, LANES // 2).transpose(0, 2, 1, 3)
    main, rest = main.reshape(n_x * block, -1), rest.reshape(n_x * block, -1)
    over = columns % LANES
    tiled = jnp.tile(rest[:, over : over + RANK].astype(bf16), (1, own // RANK))
    of_member = np.arange(n_x * block)[:, None] // MEMBER_TOKENS == np.arange(own) // RANK
    spread = tiled * jnp.asarray(of_member, bf16)
    correction = jnp.dot(spread, right_factors, preferred_element_type=f32)
    hidden = (jnp.concatenate([main, rest[:, :over]], 1) + MIXING * correction).astype(bf16)

    turn, z_core = jnp.arange(2 * n_hi) % n_hi, jnp.arange(2 * n_hi) // n_hi
    z = 2 * ((hi + turn) % n_hi) + jnp.where(z_core == 1, core, 1 - core)
    member = ((z[:, None] * n_x + x) * n_lo + jnp.arange(n_lo)) * (rows // MEMBER_TOKENS)
    member = member[:, :, None] + jnp.arange(factors) // RANK
    fit = jnp.sum(jnp.where(member[..., None] == jnp.arange(fitness.shape[0]), fitness, 0.0), -1)
    weighted = (fit[..., None] * near_left[:, :, :factors].astype(f32)).astype(bf16).reshape(-1, features)
    lefts = [weighted] + [shifted(weighted, "x", -j) for j in range(1, n_x)]
    lefts = jnp.stack(lefts + lefts[:-1])
    lefts = lax.dynamic_slice_in_dim(lefts, (n_x - x) % n_x, n_x)
    lefts = lefts.reshape(n_x, 2, n_hi, n_lo * factors, features).transpose(1, 2, 0, 3, 4).reshape(2, -1, features)
    gradient = 0.0
    for left, right in zip(lefts, (right_other, right_same)):
        gradient += jnp.einsum("kd,kf->df", left, right.reshape(-1, columns), preferred_element_type=f32)
    return hidden, (gradient * GRADIENT_SCALE).astype(bf16)


def solution(mesh):
    finer = Mesh(mesh.devices.reshape(8, 4, 2, 4, 2), MEMBER + TENSOR)
    return jax.shard_map(
        body,
        mesh=finer,
        in_specs=(P(MEMBER, TENSOR), P(TENSOR, MEMBER), P(MEMBER, TENSOR), P(TENSOR, MEMBER), P()),
        out_specs=(P(TENSOR, MEMBER), P(TENSOR, MEMBER)),
        check_vma=False,
    )
```
